512 devices in a mesh: depth: 64 (over x, y, core), samp: 8 (over z).
Axes of the slice: x: 4, y: 8, z: 8, core: 2. Of those that a mesh axis runs over, the one named last changes fastest.
Arguments:
- activations: bfloat16 [8, 64, 64, 16, 128], P('samp', 'depth'), may hold values from -6 to 6
- preact: bfloat16 [8, 64, 64, 16, 128], P('samp', 'depth'), may hold values from -6 to 6
- out_grad: bfloat16 [8, 64, 64, 16, 128], P('samp', 'depth'), may hold values from -6 to 6
- weights: bfloat16 [3, 3, 3, 128, 128], replicated, may hold values from -0.109375 to 0.109375
- master: float32 [442368], P(('depth', 'samp')), may hold values from -0.109375 to 0.109375
- moment: float32 [442368], P(('depth', 'samp')), may hold values from -4 to 4
- second: float32 [442368], P(('depth', 'samp')), may hold values from 0.1 to 1
Outputs:
- grad_input: bfloat16 [8, 64, 64, 16, 128], P('samp', 'depth')
- filter_grad: float32 [442368], P(('depth', 'samp'))
- new_moment: float32 [442368], P(('depth', 'samp'))
- new_second: float32 [442368], P(('depth', 'samp'))
- new_master: float32 [442368], P(('depth', 'samp'))
- new_weights: bfloat16 [3, 3, 3, 128, 128], replicated
The draws below stay inside these ranges and needn't reach their ends.
All inputs are finite; a program needn't handle non-finite values.
Results may differ from the reference program's by a relative error of at most 0.001.
Values may be sent and summed in bfloat16 or wider, within the bound.
A program may use at most 64 MiB of HBM per device.

```python
import math
import jax
import jax.numpy as jnp
from jax import lax

CH = 128
HEIGHT = 64
WIDTH = 16
DEPTH = 64
SAMPLES = 8
PARAMS = 442368


def levels(rng, extent, shards, least, top_value):
    def one(axis_at, parts):
        draws = jax.random.uniform(jax.random.fold_in(jax.random.fold_in(rng, 6), axis_at), (parts,), jnp.float32, least / len(shards), top_value / len(shards))
        return jnp.repeat(jnp.exp(draws), extent[axis_at] // parts).reshape((-1,) + (1,) * (len(extent) - axis_at - 1))

    level = one(*shards[0])
    for cut in shards[1:]:
        level = level * one(*cut)
    return level


def bell_draw(stream_key, shape, scale, limit, shards=(), kind=jnp.bfloat16):
    entries = jax.random.normal(stream_key, shape, jnp.float32) * scale
    if len(shards) > 0:
        entries = levels(stream_key, shape, shards, -0.22, 0.18) * entries
    return jnp.clip(entries, min=-limit, max=limit).astype(kind)


def setup_inputs(seed: int = 0) -> dict:
    keys = jax.random.split(jax.random.key(seed), 8)
    activations = bell_draw(keys[0], (SAMPLES, DEPTH, HEIGHT, WIDTH, CH), 1.0, 6.0, ((0, 8), (1, 64)))
    preact = bell_draw(keys[1], (SAMPLES, DEPTH, HEIGHT, WIDTH, CH), 1.0, 6.0, ((0, 8), (1, 64)))
    out_grad = bell_draw(keys[2], (SAMPLES, DEPTH, HEIGHT, WIDTH, CH), 1.0, 6.0, ((0, 8), (1, 64)))
    weights = bell_draw(keys[3], (3, 3, 3, CH, CH), (27 * CH) ** -0.5, 0.109375)
    master = bell_draw(keys[4], (PARAMS,), (27 * CH) ** -0.5, 0.109375, ((0, 512),), jnp.float32)
    moment = bell_draw(keys[5], (PARAMS,), 0.5, 4.0, ((0, 512),), jnp.float32)
    second = jnp.clip(jnp.exp(math.log(1.0) - 2.3025851 * jax.random.uniform(keys[6], (PARAMS,), jnp.float32) ** levels(keys[6], (PARAMS,), ((0, 512),), -0.2, 0.2)), 0.1, 1.0)
    return dict(activations=activations, preact=preact, out_grad=out_grad, weights=weights, master=master, moment=moment, second=second)


first_fix = 1.0
second_fix = 0.63230457524

def reference(activations, preact, out_grad, weights, master, moment, second):
    planes = activations.shape[1]
    height = activations.shape[2]
    width = activations.shape[3]
    chans = activations.shape[4]
    count = activations.shape[0] * planes * height * width
    widths = ((1, 1), (1, 1), (1, 1), (0, 0))

    def per_sample(total, item):
        source, before, upstream = item
        slope = jnp.where(before > 0, jnp.float32(1.0), jnp.float32(0.01))
        cotangent = (upstream.astype(jnp.float32) * slope).astype(jnp.bfloat16)
        padded_cot = jnp.pad(cotangent, widths)
        padded_src = jnp.pad(source, widths)
        flat_cot = cotangent.reshape(-1, chans)
        result = jnp.zeros((planes * height * width, chans), jnp.float32)
        terms = []
        for depth_tap in range(3):
            for row_tap in range(3):
                for col_tap in range(3):
                    cot_part = padded_cot[2 - depth_tap:2 - depth_tap + planes, 2 - row_tap:2 - row_tap + height, 2 - col_tap:2 - col_tap + width]
                    result = result + jnp.dot(cot_part.reshape(-1, chans), weights[depth_tap, row_tap, col_tap].T, preferred_element_type=jnp.float32)
                    src_part = padded_src[depth_tap:depth_tap + planes, row_tap:row_tap + height, col_tap:col_tap + width]
                    terms.append(jnp.dot(src_part.reshape(-1, chans).T, flat_cot, preferred_element_type=jnp.float32))
        return (total + jnp.stack(terms), result.reshape(planes, height, width, chans).astype(jnp.bfloat16))
    start = jnp.zeros((27, chans, chans), jnp.float32)
    raw, grad_input = lax.scan(per_sample, start, (activations, preact, out_grad))
    filter_grad = raw.reshape(-1) * jnp.float32(1.0 / count ** 0.5)
    new_moment = 0.9 * moment + 0.1 * filter_grad
    new_second = 0.999 * second + 0.001 * filter_grad * filter_grad
    new_master = master - 0.01 * (new_moment / first_fix) / (jnp.sqrt(new_second / second_fix) + 1e-08)
    new_weights = new_master.astype(jnp.bfloat16).reshape(3, 3, 3, chans, chans)
    return (grad_input, filter_grad, new_moment, new_second, new_master, new_weights)
```

```python
import jax
import jax.numpy as jnp
from jax import lax
from jax.experimental import pallas as pl
from jax.experimental.pallas import tpu as pltpu
from jax.sharding import PartitionSpec as P

first_fix = 1.0
second_fix = 0.63230457524

NX, NY, NC, NZ = 4, 8, 2, 8
H, W, CH = 64, 16, 128
POS = H * W
ROWS = 54
PAD = 56
SHARE = 864
COUNT = 8 * 64 * H * W
MESH = pl.DeviceIdType.MESH


def first_row(z):
    return (27 * z) // 4


def kernel(
    act_hbm, pre_hbm, og_hbm, w_hbm, opt_ref,
    gi_ref, fg_ref, nm_ref, ns_ref, nma_ref, nw_ref,
    act, pre, og, wts, in_sem,
    cc, halo, halo_s, halo_r,
    xs, act_t, flat, grid,
    r0, r0_s, r0_r,
    s1, r1, r1_s, r1_r,
    s2, r2, r2_s, r2_r,
    s3, win, r3, r3_s, r3_r,
    out_win, r4, r4_s, r4_r, block,
    full, y_s, y_r, x_s, x_r, c_s, c_r,
):
    p = lax.axis_index("depth")
    z = lax.axis_index("samp")
    n_depth = NX * NY * NC
    c = lax.rem(p, NC)
    y = lax.rem(p // NC, NY)
    x = p // (NC * NY)

    def dev(xx, yy, ccore, zz):
        return {"depth": (xx * NY + yy) * NC + ccore, "samp": zz}

    below = {"depth": lax.rem(p + n_depth - 1, n_depth), "samp": z}
    above = {"depth": lax.rem(p + 1, n_depth), "samp": z}
    partner = dev(x, y, 1 - c, z)
    x_peer = [dev(lax.rem(x + k, NX), y, c, z) for k in range(NX)]
    y_peer = [dev(x, lax.rem(y + k, NY), c, z) for k in range(NY)]
    z_peer = [dev(x, y, c, lax.rem(z + k, NZ)) for k in range(NZ)]

    barrier = pltpu.get_barrier_semaphore()
    peers = [below, above] + x_peer[1:] + y_peer[1:] + z_peer[1:]
    for peer in peers:
        pl.semaphore_signal(barrier, inc=1, device_id=peer, device_id_type=MESH)

    loads = [
        pltpu.make_async_copy(src, dst, in_sem.at[i])
        for i, (src, dst) in enumerate(
            ((pre_hbm, pre), (og_hbm, og), (act_hbm, act), (w_hbm, wts))
        )
    ]
    for load in loads:
        load.start()
    loads[0].wait()
    loads[1].wait()

    @pl.loop(0, 8)
    def _(i):
        part = pl.ds(i * 8, 8)
        slope = jnp.where(pre[part].astype(jnp.float32) > 0, jnp.float32(1.0), jnp.float32(0.01))
        cc[part] = (og[part].astype(jnp.float32) * slope).astype(jnp.bfloat16)

    pl.semaphore_wait(barrier, len(peers))

    def remote(src, dst, s, r, to):
        return pltpu.make_async_remote_copy(
            src_ref=src, dst_ref=dst, send_sem=s, recv_sem=r, device_id=to, device_id_type=MESH
        )

    halo_copies = [
        remote(cc, halo.at[0], halo_s.at[0], halo_r.at[0], above),
        remote(cc, halo.at[1], halo_s.at[1], halo_r.at[1], below),
    ]
    for copy in halo_copies:
        copy.start()

    def spread(src, plane, keep):
        zero_row = jnp.zeros((W, CH), jnp.bfloat16)
        for col in range(3):
            xs[col, plane, 0] = zero_row
            xs[col, plane, H + 1] = zero_row

        @pl.loop(0, 8)
        def _(i):
            v = src[pl.ds(i * 8, 8)].astype(jnp.float32).reshape(8 * W, CH)
            if keep is not None:
                v = jnp.where(keep, v, 0.0)
            w = lax.broadcasted_iota(jnp.int32, (8 * W, CH), 0) % W
            after = jnp.where(w == W - 1, 0.0, pltpu.roll(v, 8 * W - 1, 0))
            before = jnp.where(w == 0, 0.0, pltpu.roll(v, 1, 0))
            for col, moved in ((0, after), (1, v), (2, before)):
                xs[col, plane, pl.ds(1 + i * 8, 8)] = moved.reshape(8, W, CH).astype(jnp.bfloat16)

    def taps(a):
        @pl.loop(0, 3)
        def _(b):
            right = jnp.concatenate(
                [xs[col, 2 - a, pl.ds(2 - b, H)].reshape(POS, CH) for col in range(3)], axis=1
            )
            raw = jnp.dot(act_t[...], right, preferred_element_type=jnp.float32)
            for col in range(3):
                row = pl.multiple_of(((a * 3 + b) * 3 + col) * CH, CH)
                flat[pl.ds(row, CH)] = raw[:, col * CH : (col + 1) * CH]

    loads[2].wait()
    act_t[...] = act[...].reshape(POS, CH).astype(jnp.float32).T.astype(jnp.bfloat16)
    spread(cc, 1, None)
    taps(1)
    halo_copies[0].wait_recv()
    spread(halo.at[0], 0, p > 0)
    taps(2)
    halo_copies[1].wait_recv()
    spread(halo.at[1], 2, p < n_depth - 1)
    taps(0)

    core_copies = []
    for xx in range(NX):

        @pl.loop(0, NY)
        def _(yy):
            for cr in range(NC):
                start = ((xx * NY + yy) * NC + cr) * ROWS
                grid[cr, xx, yy, 0:ROWS] = flat[pl.ds(start, ROWS)]

        copy = remote(grid.at[1 - c, xx], r0.at[xx], r0_s.at[xx], r0_r.at[xx], partner)
        copy.start()
        core_copies.append(copy)
    for xx in range(NX):
        core_copies[xx].wait_recv()

        @pl.loop(0, NY)
        def _(yy):
            s1[xx, yy] = grid[c, xx, yy] + r0[xx, yy]

    x_copies = []
    for k in (2, 1, 3):
        copy = remote(
            s1.at[lax.rem(x + k, NX)], r1.at[k - 1], r1_s.at[k - 1], r1_r.at[k - 1], x_peer[k]
        )
        copy.start()
        x_copies.append(copy)

    loads[3].wait()

    @pl.loop(0, 4)
    def _(m):
        acc = jnp.zeros((POS // 4, CH), jnp.float32)
        for a in range(3):
            for b in range(3):
                left = jnp.concatenate(
                    [
                        xs[col, 2 - a, pl.ds(2 - b + m * (H // 4), H // 4)].reshape(POS // 4, CH)
                        for col in range(3)
                    ],
                    axis=1,
                )
                right = jnp.concatenate([wts[(a * 3 + b) * 3 + col] for col in range(3)], axis=1)
                acc = acc + lax.dot_general(
                    left, right, (((1,), (1,)), ((), ())), preferred_element_type=jnp.float32
                )
        gi_ref[pl.ds(m * (H // 4), H // 4)] = acc.reshape(H // 4, W, CH).astype(jnp.bfloat16)

    for copy in x_copies:
        copy.wait_recv()

    @pl.loop(0, NY)
    def _(yy):
        s2[yy] = s1[x, yy] + r1[0, yy] + r1[1, yy] + r1[2, yy]

    y_copies = []
    for k in (4, 3, 5, 2, 6, 1, 7):
        copy = remote(
            s2.at[lax.rem(y + k, NY)], r2.at[k - 1], r2_s.at[k - 1], r2_r.at[k - 1], y_peer[k]
        )
        copy.start()
        y_copies.append(copy)
    for copy in y_copies:
        copy.wait_recv()
    total = s2[y]
    for k in range(1, NY):
        total = total + r2[k - 1]
    s3[...] = total

    for zz in range(NZ):
        win[zz] = s3[first_row(zz) : first_row(zz) + 8]
    z_copies = []
    for k in (4, 3, 5, 2, 6, 1, 7):
        copy = remote(
            win.at[lax.rem(z + k, NZ)], r3.at[k - 1], r3_s.at[k - 1], r3_r.at[k - 1], z_peer[k]
        )
        copy.start()
        z_copies.append(copy)
    for copy in z_copies:
        copy.wait_recv()
    raw = win[z]
    for k in range(1, NZ):
        raw = raw + r3[k - 1]

    off = lax.rem(96 * z, 128)
    lane = lax.broadcasted_iota(jnp.int32, (8, CH), 1)
    row = lax.broadcasted_iota(jnp.int32, (8, CH), 0)
    turned = pltpu.roll(raw, lax.rem(128 - off, 128), 1)
    raw = jnp.where(lane < 128 - off, turned, pltpu.roll(turned, 7, 0))
    filter_grad = raw * jnp.float32(1.0 / COUNT**0.5)
    new_moment = 0.9 * opt_ref[1] + 0.1 * filter_grad
    new_second = 0.999 * opt_ref[2] + 0.001 * filter_grad * filter_grad
    new_master = opt_ref[0] - 0.01 * (new_moment / first_fix) / (
        jnp.sqrt(new_second / second_fix) + 1e-08
    )
    fg_ref[...] = filter_grad
    nm_ref[...] = new_moment
    ns_ref[...] = new_second
    nma_ref[...] = new_master

    turned = pltpu.roll(new_master, off, 1)
    moved = jnp.where(lane >= off, turned, pltpu.roll(turned, 1, 0))
    place = row * CH + lane
    mine = jnp.where((place >= off) & (place < off + SHARE), moved, 0.0)
    out_win[...] = mine
    r4[z] = mine
    share_copies = []
    for k in (4, 3, 5, 2, 6, 1, 7):
        copy = remote(out_win, r4.at[z], r4_s.at[k - 1], r4_r.at[k - 1], z_peer[k])
        copy.start()
        share_copies.append(copy)
    for copy in share_copies:
        copy.wait_recv()
    block[...] = jnp.zeros_like(block)
    for zz in range(NZ):
        part = pl.ds(first_row(zz), 8)
        block[part] = block[part] + r4[zz]
    full[c, x, y] = block[0:PAD].astype(jnp.bfloat16)

    gather_y = []
    for k in (4, 3, 5, 2, 6, 1, 7):
        copy = remote(
            full.at[c, x, y], full.at[c, x, y], y_s.at[k - 1], y_r.at[k - 1], y_peer[k]
        )
        copy.start()
        gather_y.append(copy)
    for copy in gather_y:
        copy.wait_recv()

    gather_x = {}
    for k in (2, 1, 3):
        gather_x[k] = remote(full.at[c, x], full.at[c, x], x_s.at[k - 1], x_r.at[k - 1], x_peer[k])
        gather_x[k].start()
    gather_c = []
    for k in (0, 1, 3, 2):
        if k:
            gather_x[k].wait_recv()
        came = lax.rem(x + NX - k, NX)
        copy = remote(full.at[c, came], full.at[c, came], c_s.at[k], c_r.at[k], partner)
        copy.start()
        gather_c.append(copy)
    for copy in gather_c:
        copy.wait_recv()
    for xx in range(NX):
        for yy in range(NY):
            for cr in range(NC):
                start = ((xx * NY + yy) * NC + cr) * ROWS
                nw_ref[start : start + ROWS] = full[cr, xx, yy, 0:ROWS]

    sends = halo_copies + core_copies + x_copies + y_copies + z_copies + share_copies
    for copy in sends + gather_y + list(gather_x.values()) + gather_c:
        copy.wait_send()


def step(activations, preact, out_grad, weights, opt):
    vmem = pl.BlockSpec(memory_space=pltpu.VMEM)
    hbm = pl.BlockSpec(memory_space=pl.ANY)
    f32, bf16 = jnp.float32, jnp.bfloat16
    dma = pltpu.SemaphoreType.DMA
    shape = jax.ShapeDtypeStruct
    return pl.pallas_call(
        kernel,
        out_shape=(
            shape((H, W, CH), bf16),
            shape((8, CH), f32),
            shape((8, CH), f32),
            shape((8, CH), f32),
            shape((8, CH), f32),
            shape((NX * NY * NC * ROWS, CH), bf16),
        ),
        in_specs=[hbm, hbm, hbm, hbm, vmem],
        out_specs=(vmem,) * 6,
        scratch_shapes=[
            pltpu.VMEM((H, W, CH), bf16),
            pltpu.VMEM((H, W, CH), bf16),
            pltpu.VMEM((H, W, CH), bf16),
            pltpu.VMEM((27, CH, CH), bf16),
            dma((4,)),
            pltpu.VMEM((H, W, CH), bf16),
            pltpu.VMEM((2, H, W, CH), bf16),
            dma((2,)),
            dma((2,)),
            pltpu.VMEM((3, 3, H + 2, W, CH), bf16),
            pltpu.VMEM((CH, POS), bf16),
            pltpu.VMEM((NX * NY * NC * ROWS, CH), f32),
            pltpu.VMEM((NC, NX, NY, PAD, CH), f32),
            pltpu.VMEM((NX, NY, PAD, CH), f32),
            dma((NX,)),
            dma((NX,)),
            pltpu.VMEM((NX, NY, PAD, CH), f32),
            pltpu.VMEM((NX - 1, NY, PAD, CH), f32),
            dma((NX - 1,)),
            dma((NX - 1,)),
            pltpu.VMEM((NY, PAD, CH), f32),
            pltpu.VMEM((NY - 1, PAD, CH), f32),
            dma((NY - 1,)),
            dma((NY - 1,)),
            pltpu.VMEM((PAD, CH), f32),
            pltpu.VMEM((NZ, 8, CH), f32),
            pltpu.VMEM((NZ - 1, 8, CH), f32),
            dma((NZ - 1,)),
            dma((NZ - 1,)),
            pltpu.VMEM((8, CH), f32),
            pltpu.VMEM((NZ, 8, CH), f32),
            dma((NZ - 1,)),
            dma((NZ - 1,)),
            pltpu.VMEM((64, CH), f32),
            pltpu.VMEM((NC, NX, NY, PAD, CH), bf16),
            dma((NY - 1,)),
            dma((NY - 1,)),
            dma((NX - 1,)),
            dma((NX - 1,)),
            dma((NX,)),
            dma((NX,)),
        ],
        compiler_params=pltpu.CompilerParams(
            collective_id=0, has_side_effects=True, vmem_limit_bytes=40 * 1024 * 1024
        ),
        name="conv_step",
    )(activations, preact, out_grad, weights, opt)


def local(activations, preact, out_grad, weights, master, moment, second):
    plane = (H, W, CH)
    opt = jnp.pad(jnp.stack([master, moment, second]), ((0, 0), (0, 8 * CH - SHARE)))
    gi, fg, nm, ns, nma, nw = step(
        activations.reshape(plane),
        preact.reshape(plane),
        out_grad.reshape(plane),
        weights.reshape(27, CH, CH),
        opt.reshape(3, 8, CH),
    )
    own = [a.reshape(-1)[:SHARE] for a in (fg, nm, ns, nma)]
    return (gi.reshape(activations.shape), *own, nw.reshape(weights.shape))


def solution(mesh):
    volume = P("samp", "depth", None, None, None)
    shares = P(("depth", "samp"))
    return jax.shard_map(
        local,
        mesh=mesh,
        in_specs=(volume, volume, volume, P(), shares, shares, shares),
        out_specs=(volume, shares, shares, shares, shares, P()),
        check_vma=False,
    )
```

```python
import jax
import jax.numpy as jnp
from jax import lax
from jax.experimental import pallas as pl
from jax.experimental.pallas import tpu as pltpu
from jax.sharding import PartitionSpec as P

first_fix = 1.0
second_fix = 0.63230457524

NX, NY, NC, NZ = 4, 8, 2, 8
H, W, CH = 64, 16, 128
POS = H * W
ROWS = 54
PAD = 56
SHARE = 864
COUNT = 8 * 64 * H * W
MESH = pl.DeviceIdType.MESH


def first_row(z):
    return (27 * z) // 4


def kernel(
    act_hbm, pre_hbm, og_hbm, w_hbm, ma_hbm, mo_hbm, se_hbm,
    gi_ref, fg_ref, nm_ref, ns_ref, nma_ref, nw_ref,
    act, pre, og, wts, ma, mo, se, in_sem,
    cc, halo, halo_s, halo_r,
    xs, act_t, flat, give,
    r0, r0_s, r0_r,
    s1, rel, rel_s, rel_r, r1, near_s, near_r, relayed, sum_s, sum_r,
    s2, r2, r2_s, r2_r,
    s3, win, r3, r3_s, r3_r,
    out_win, r4, r4_s, r4_r, block,
    full, y_s, y_r, up_s, up_r, dn_s, dn_r, fw_s, fw_r, c_s, c_r,
):
    p = lax.axis_index("depth")
    z = lax.axis_index("samp")
    n_depth = NX * NY * NC
    c = lax.rem(p, NC)
    y = lax.rem(p // NC, NY)
    x = p // (NC * NY)

    def dev(xx, yy, ccore, zz):
        return {"depth": (xx * NY + yy) * NC + ccore, "samp": zz}

    below = {"depth": lax.rem(p + n_depth - 1, n_depth), "samp": z}
    above = {"depth": lax.rem(p + 1, n_depth), "samp": z}
    partner = dev(x, y, 1 - c, z)
    xk = [lax.rem(x + k, NX) for k in range(NX)]
    x_up = dev(xk[1], y, c, z)
    x_dn = dev(xk[3], y, c, z)
    y_peer = [dev(x, lax.rem(y + k, NY), c, z) for k in range(NY)]
    z_peer = [dev(x, y, c, lax.rem(z + k, NZ)) for k in range(NZ)]

    loads = [
        pltpu.make_async_copy(src, dst, in_sem.at[i])
        for i, (src, dst) in enumerate(
            (
                (pre_hbm, pre),
                (og_hbm, og),
                (act_hbm, act),
                (w_hbm, wts),
                (ma_hbm, ma),
                (mo_hbm, mo),
                (se_hbm, se),
            )
        )
    ]
    for load in loads:
        load.start()

    barrier = pltpu.get_barrier_semaphore()
    peers = [below, above, x_up, x_dn] + y_peer[1:] + z_peer[1:]
    for peer in peers:
        pl.semaphore_signal(barrier, inc=1, device_id=peer, device_id_type=MESH)

    loads[0].wait()
    loads[1].wait()

    @pl.loop(0, 8)
    def _(i):
        part = pl.ds(i * 8, 8)
        slope = jnp.where(pre[part].astype(jnp.float32) > 0, jnp.float32(1.0), jnp.float32(0.01))
        cc[part] = (og[part].astype(jnp.float32) * slope).astype(jnp.bfloat16)

    pl.semaphore_wait(barrier, len(peers))

    started = []

    def remote(src, dst, s, r, to):
        copy = pltpu.make_async_remote_copy(
            src_ref=src, dst_ref=dst, send_sem=s, recv_sem=r, device_id=to, device_id_type=MESH
        )
        copy.start()
        started.append(copy)
        return copy

    from_below = remote(cc, halo.at[0], halo_s.at[0], halo_r.at[0], above)
    from_above = remote(cc, halo.at[1], halo_s.at[1], halo_r.at[1], below)

    def spread(src, plane, keep):
        zero_row = jnp.zeros((W, CH), jnp.bfloat16)
        for col in range(3):
            xs[col, plane, 0] = zero_row
            xs[col, plane, H + 1] = zero_row

        @pl.loop(0, 8)
        def _(i):
            v = src[pl.ds(i * 8, 8)].astype(jnp.float32).reshape(8 * W, CH)
            if keep is not None:
                v = jnp.where(keep, v, 0.0)
            w = lax.broadcasted_iota(jnp.int32, (8 * W, CH), 0) % W
            after = jnp.where(w == W - 1, 0.0, pltpu.roll(v, 8 * W - 1, 0))
            before = jnp.where(w == 0, 0.0, pltpu.roll(v, 1, 0))
            for col, moved in ((0, after), (1, v), (2, before)):
                xs[col, plane, pl.ds(1 + i * 8, 8)] = moved.reshape(8, W, CH).astype(jnp.bfloat16)

    def taps(a):
        @pl.loop(0, 3)
        def _(b):
            right = jnp.concatenate(
                [xs[col, 2 - a, pl.ds(2 - b, H)].reshape(POS, CH) for col in range(3)], axis=1
            )
            raw = jnp.dot(act_t[...], right, preferred_element_type=jnp.float32)
            for col in range(3):
                row = pl.multiple_of(((a * 3 + b) * 3 + col) * CH, CH)
                flat[pl.ds(row, CH)] = raw[:, col * CH : (col + 1) * CH]

    loads[2].wait()
    act_t[...] = act[...].reshape(POS, CH).astype(jnp.float32).T.astype(jnp.bfloat16)
    spread(cc, 1, None)
    taps(1)
    from_below.wait_recv()
    spread(halo.at[0], 0, p > 0)
    taps(2)
    from_above.wait_recv()
    spread(halo.at[1], 2, p < n_depth - 1)
    taps(0)

    core_copies = {}
    for k in (2, 1, 3, 0):
        xx = xk[k]

        @pl.loop(0, NY)
        def _(yy):
            give[xx, yy, 0:ROWS] = flat[pl.ds(((xx * NY + yy) * NC + 1 - c) * ROWS, ROWS)]

        core_copies[k] = remote(give.at[xx], r0.at[xx], r0_s.at[k], r0_r.at[k], partner)

    def both_cores(k):
        xx = xk[k]
        core_copies[k].wait_recv()

        @pl.loop(0, NY)
        def _(yy):
            own = flat[pl.ds(((xx * NY + yy) * NC + c) * ROWS, ROWS)]
            s1[xx, yy, 0:ROWS] = own + r0[xx, yy, 0:ROWS]

    order = (4, 3, 5, 2, 6, 1, 7, 0)
    by_down = {k: i % 2 == 0 for i, k in enumerate(order)}
    yk = [lax.rem(y + k, NY) for k in range(NY)]
    relays, nears, sums = {}, {}, {}
    both_cores(2)
    for k in order:
        to = x_dn if by_down[k] else x_up
        relays[k] = remote(s1.at[xk[2], yk[k]], rel.at[k], rel_s.at[k], rel_r.at[k], to)
    both_cores(1)
    both_cores(3)

    def near(k):
        if by_down[k]:
            nears[k] = remote(s1.at[xk[1], yk[k]], r1.at[0, k], near_s.at[k], near_r.at[k], x_up)
        else:
            nears[k] = remote(s1.at[xk[3], yk[k]], r1.at[1, k], near_s.at[k], near_r.at[k], x_dn)

    near(order[0])
    near(order[1])
    both_cores(0)

    loads[3].wait()

    @pl.loop(0, 4)
    def _(m):
        acc = jnp.zeros((POS // 4, CH), jnp.float32)
        for a in range(3):
            for b in range(3):
                left = jnp.concatenate(
                    [
                        xs[col, 2 - a, pl.ds(2 - b + m * (H // 4), H // 4)].reshape(POS // 4, CH)
                        for col in range(3)
                    ],
                    axis=1,
                )
                right = jnp.concatenate([wts[(a * 3 + b) * 3 + col] for col in range(3)], axis=1)
                acc = acc + lax.dot_general(
                    left, right, (((1,), (1,)), ((), ())), preferred_element_type=jnp.float32
                )
        gi_ref[pl.ds(m * (H // 4), H // 4)] = acc.reshape(H // 4, W, CH).astype(jnp.bfloat16)

    y_copies = {}

    def root(k):
        nears[k].wait_recv()
        sums[k].wait_recv()
        s2[k] = s1[x, yk[k]] + r1[0, k] + r1[1, k]
        if k:
            y_copies[k] = remote(
                s2.at[k], r2.at[k - 1], r2_s.at[k - 1], r2_r.at[k - 1], y_peer[k]
            )

    for i, k in enumerate(order):
        if i + 2 < NY:
            near(order[i + 2])
        relays[k].wait_recv()
        if by_down[k]:
            relayed[k] = s1[xk[3], yk[k]] + rel[k]
            sums[k] = remote(relayed.at[k], r1.at[1, k], sum_s.at[k], sum_r.at[k], x_dn)
        else:
            relayed[k] = s1[xk[1], yk[k]] + rel[k]
            sums[k] = remote(relayed.at[k], r1.at[0, k], sum_s.at[k], sum_r.at[k], x_up)
        if i >= 3:
            root(order[i - 3])
    for k in order[-3:]:
        root(k)

    total = s2[0]
    for k in (7, 1, 6, 2, 5, 3, 4):
        y_copies[k].wait_recv()
        total = total + r2[k - 1]
    s3[...] = total

    for zz in range(NZ):
        win[zz] = s3[first_row(zz) : first_row(zz) + 8]
    far_first = (4, 3, 5, 2, 6, 1, 7)
    z_copies = [
        remote(win.at[lax.rem(z + k, NZ)], r3.at[k - 1], r3_s.at[k - 1], r3_r.at[k - 1], z_peer[k])
        for k in far_first
    ]
    for copy in z_copies:
        copy.wait_recv()
    raw = win[z]
    for k in range(1, NZ):
        raw = raw + r3[k - 1]

    for load in loads[4:]:
        load.wait()
    off = lax.rem(96 * z, 128)
    lane = lax.broadcasted_iota(jnp.int32, (8, CH), 1)
    row = lax.broadcasted_iota(jnp.int32, (8, CH), 0)
    turned = pltpu.roll(raw, lax.rem(128 - off, 128), 1)
    raw = jnp.where(lane < 128 - off, turned, pltpu.roll(turned, 7, 0))
    filter_grad = raw * jnp.float32(1.0 / COUNT**0.5)

    def wide(ref):
        return jnp.concatenate([ref[...], jnp.zeros((8 * CH - SHARE,), jnp.float32)]).reshape(8, CH)

    new_moment = 0.9 * wide(mo) + 0.1 * filter_grad
    new_second = 0.999 * wide(se) + 0.001 * filter_grad * filter_grad
    new_master = wide(ma) - 0.01 * (new_moment / first_fix) / (
        jnp.sqrt(new_second / second_fix) + 1e-08
    )

    turned = pltpu.roll(new_master, off, 1)
    moved = jnp.where(lane >= off, turned, pltpu.roll(turned, 1, 0))
    place = row * CH + lane
    mine = jnp.where((place >= off) & (place < off + SHARE), moved, 0.0)
    out_win[...] = mine
    r4[z] = mine
    share_copies = [
        remote(out_win, r4.at[z], r4_s.at[k - 1], r4_r.at[k - 1], z_peer[k]) for k in far_first
    ]
    fg_ref[...] = filter_grad
    nm_ref[...] = new_moment
    ns_ref[...] = new_second
    nma_ref[...] = new_master
    block[...] = jnp.zeros_like(block)
    for copy in share_copies:
        copy.wait_recv()
    for zz in range(NZ):
        part = pl.ds(first_row(zz), 8)
        block[part] = block[part] + r4[zz]
    full[c, x, y] = block[0:PAD].astype(jnp.bfloat16)

    gather_y = {}
    for k in far_first:
        gather_y[k] = remote(
            full.at[c, x, y], full.at[c, x, y], y_s.at[k - 1], y_r.at[k - 1], y_peer[k]
        )
    near_first = (0, 1, 7, 2, 6, 3, 5, 4)
    up, down, onward, gather_c = {}, {}, {}, {}

    def to_partner(k):
        part = full.at[c, xk[k]]
        gather_c[k] = remote(part, part, c_s.at[k], c_r.at[k], partner)

    src_y = [lax.rem(y + NY - k, NY) for k in range(NY)]
    for k in near_first:
        if k:
            gather_y[k].wait_recv()
        part = full.at[c, x, src_y[k]]
        up[k] = remote(part, part, up_s.at[k], up_r.at[k], x_up)
        down[k] = remote(part, part, dn_s.at[k], dn_r.at[k], x_dn)
    to_partner(0)
    for i, k in enumerate(near_first):
        up[k].wait_recv()
        down[k].wait_recv()
        if i % 2 == 0:
            part = full.at[c, xk[3], src_y[k]]
            onward[k] = remote(part, part, fw_s.at[k], fw_r.at[k], x_up)
        else:
            part = full.at[c, xk[1], src_y[k]]
            onward[k] = remote(part, part, fw_s.at[k], fw_r.at[k], x_dn)
    to_partner(3)
    to_partner(1)

    def lay_out(k):
        xx = xk[k]
        gather_c[k].wait_recv()
        for yy in range(NY):
            for cr in range(NC):
                start = (yy * NC + cr) * ROWS
                nw_ref[xx, start : start + ROWS] = full[cr, xx, yy, 0:ROWS]

    lay_out(0)
    lay_out(3)
    lay_out(1)
    for k in near_first:
        onward[k].wait_recv()
    to_partner(2)
    lay_out(2)

    for copy in started:
        copy.wait_send()


def write_kernel(gi, fg, nm, ns, nma, nw, gi_o, fg_o, nm_o, ns_o, nma_o, nw_o, sem):
    copies = [
        pltpu.make_async_copy(src, dst, sem.at[i])
        for i, (src, dst) in enumerate(
            ((nw, nw_o), (gi, gi_o), (fg, fg_o), (nm, nm_o), (ns, ns_o), (nma, nma_o))
        )
    ]
    for copy in copies:
        copy.start()
    for copy in copies:
        copy.wait()


def step(*operands):
    vmem = pl.BlockSpec(memory_space=pltpu.VMEM)
    hbm = pl.BlockSpec(memory_space=pltpu.HBM)
    f32, bf16 = jnp.float32, jnp.bfloat16
    shape = jax.ShapeDtypeStruct

    def dma(n):
        return pltpu.SemaphoreType.DMA((n,))

    plane = pltpu.VMEM((H, W, CH), bf16)
    return pl.pallas_call(
        kernel,
        out_shape=(
            shape((H, W, CH), bf16),
            shape((8, CH), f32),
            shape((8, CH), f32),
            shape((8, CH), f32),
            shape((8, CH), f32),
            shape((NX, NY * NC * ROWS, CH), bf16),
        ),
        in_specs=[hbm] * 7,
        out_specs=(vmem,) * 6,
        scratch_shapes=[
            plane,
            plane,
            plane,
            pltpu.VMEM((27, CH, CH), bf16),
            pltpu.VMEM((SHARE,), f32),
            pltpu.VMEM((SHARE,), f32),
            pltpu.VMEM((SHARE,), f32),
            dma(7),
            plane,
            pltpu.VMEM((2, H, W, CH), bf16),
            dma(2),
            dma(2),
            pltpu.VMEM((3, 3, H + 2, W, CH), bf16),
            pltpu.VMEM((CH, POS), bf16),
            pltpu.VMEM((NX * NY * NC * ROWS, CH), f32),
            pltpu.VMEM((NX, NY, PAD, CH), f32),
            pltpu.VMEM((NX, NY, PAD, CH), f32),
            dma(NX),
            dma(NX),
            pltpu.VMEM((NX, NY, PAD, CH), f32),
            pltpu.VMEM((NY, PAD, CH), f32),
            dma(NY),
            dma(NY),
            pltpu.VMEM((2, NY, PAD, CH), f32),
            dma(NY),
            dma(NY),
            pltpu.VMEM((NY, PAD, CH), f32),
            dma(NY),
            dma(NY),
            pltpu.VMEM((NY, PAD, CH), f32),
            pltpu.VMEM((NY - 1, PAD, CH), f32),
            dma(NY - 1),
            dma(NY - 1),
            pltpu.VMEM((PAD, CH), f32),
            pltpu.VMEM((NZ, 8, CH), f32),
            pltpu.VMEM((NZ - 1, 8, CH), f32),
            dma(NZ - 1),
            dma(NZ - 1),
            pltpu.VMEM((8, CH), f32),
            pltpu.VMEM((NZ, 8, CH), f32),
            dma(NZ - 1),
            dma(NZ - 1),
            pltpu.VMEM((64, CH), f32),
            pltpu.VMEM((NC, NX, NY, PAD, CH), bf16),
            dma(NY - 1),
            dma(NY - 1),
            dma(NY),
            dma(NY),
            dma(NY),
            dma(NY),
            dma(NY),
            dma(NY),
            dma(NX),
            dma(NX),
        ],
        compiler_params=pltpu.CompilerParams(
            collective_id=0, has_side_effects=True, vmem_limit_bytes=40 * 1024 * 1024
        ),
        name="conv_step",
    )(*[pltpu.with_memory_space_constraint(a, pltpu.HBM) for a in operands])


def write(*results):
    return pl.pallas_call(
        write_kernel,
        out_shape=tuple(jax.ShapeDtypeStruct(a.shape, a.dtype) for a in results),
        in_specs=[pl.BlockSpec(memory_space=pltpu.VMEM)] * 6,
        out_specs=(pl.BlockSpec(memory_space=pltpu.HBM),) * 6,
        scratch_shapes=[pltpu.SemaphoreType.DMA((6,))],
        compiler_params=pltpu.CompilerParams(vmem_limit_bytes=4 * 1024 * 1024),
        name="write_out",
    )(*results)


def local(activations, preact, out_grad, weights, master, moment, second):
    plane = (H, W, CH)
    opt = [master, moment, second]
    gi, fg, nm, ns, nma, nw = write(
        *step(
            activations.reshape(plane),
            preact.reshape(plane),
            out_grad.reshape(plane),
            weights.reshape(27, CH, CH),
            *opt,
        )
    )
    own = [a.reshape(-1)[:SHARE] for a in (fg, nm, ns, nma)]
    return (gi.reshape(activations.shape), *own, nw.reshape(weights.shape))


def solution(mesh):
    volume = P("samp", "depth", None, None, None)
    shares = P(("depth", "samp"))
    return jax.shard_map(
        local,
        mesh=mesh,
        in_specs=(volume, volume, volume, P(), shares, shares, shares),
        out_specs=(volume, shares, shares, shares, shares, P()),
        check_vma=False,
    )
```

```python
import jax
import jax.numpy as jnp
from jax import lax
from jax.experimental import pallas as pl
from jax.experimental.pallas import tpu as pltpu
from jax.sharding import PartitionSpec as P

first_fix = 1.0
second_fix = 0.63230457524

NX, NY, NC, NZ = 4, 8, 2, 8
H, W, CH = 64, 16, 128
POS = H * W
ROWS = 54
PAD = 56
SHARE = 864
COUNT = 8 * 64 * H * W
MESH = pl.DeviceIdType.MESH


def first_row(z):
    return (27 * z) // 4


def kernel(
    act_hbm, pre_hbm, og_hbm, w_hbm, ma_hbm, mo_hbm, se_hbm,
    gi_ref, fg_ref, nm_ref, ns_ref, nma_ref, nw_ref,
    act, pre, og, wts, ma, mo, se, in_sem,
    cc, halo, halo_s, halo_r, known,
    xs, act_t, flat, give,
    r0, r0_s, r0_r,
    s1, rel, rel_s, rel_r, r1, near_s, near_r, relayed, sum_s, sum_r,
    s2, r2, r2_s, r2_r,
    s3, win, r3, r3_s, r3_r,
    out_win, r4, r4_s, r4_r, block,
    full, y_s, y_r, up_s, up_r, dn_s, dn_r, fw_s, fw_r, c_s, c_r,
):
    p = lax.axis_index("depth")
    z = lax.axis_index("samp")
    n_depth = NX * NY * NC
    c = lax.rem(p, NC)
    y = lax.rem(p // NC, NY)
    x = p // (NC * NY)

    def dev(xx, yy, ccore, zz):
        return {"depth": (xx * NY + yy) * NC + ccore, "samp": zz}

    partner = dev(x, y, 1 - c, z)
    other = {"depth": lax.rem(p + n_depth + 2 * c - 1, n_depth), "samp": z}
    xk = [lax.rem(x + k, NX) for k in range(NX)]
    x_up = dev(xk[1], y, c, z)
    x_far = dev(xk[2], y, c, z)
    x_dn = dev(xk[3], y, c, z)
    y_peer = [dev(x, lax.rem(y + k, NY), c, z) for k in range(NY)]
    z_peer = [dev(x, y, c, lax.rem(z + k, NZ)) for k in range(NZ)]

    loads = [
        pltpu.make_async_copy(src, dst, in_sem.at[i])
        for i, (src, dst) in enumerate(
            (
                (pre_hbm, pre),
                (og_hbm, og),
                (act_hbm, act),
                (w_hbm, wts),
                (ma_hbm, ma),
                (mo_hbm, mo),
                (se_hbm, se),
            )
        )
    ]
    for load in loads:
        load.start()

    barrier = pltpu.get_barrier_semaphore()
    peers = [partner, other, x_up, x_dn, y_peer[1], y_peer[7], z_peer[1], z_peer[7]]
    for peer in peers:
        pl.semaphore_signal(barrier, inc=1, device_id=peer, device_id_type=MESH)

    loads[0].wait()
    loads[1].wait()

    @pl.loop(0, 8)
    def _(i):
        part = pl.ds(i * 8, 8)
        slope = jnp.where(pre[part].astype(jnp.float32) > 0, jnp.float32(1.0), jnp.float32(0.01))
        cc[part] = (og[part].astype(jnp.float32) * slope).astype(jnp.bfloat16)

    pl.semaphore_wait(barrier, len(peers))

    flows = ((y_peer[1], 3), (y_peer[7], 4), (z_peer[1], 3), (z_peer[7], 4), (x_up, 2))

    def pass_on(hops):
        for i, (_, last) in enumerate(flows):
            if 2 < hops <= last + 1:
                pl.semaphore_wait(known.at[i, hops - 3], 1)
        for i, (to, last) in enumerate(flows):
            if hops <= last:
                pl.semaphore_signal(
                    known.at[i, hops - 2], inc=1, device_id=to, device_id_type=MESH
                )

    started = []

    def remote(src, dst, s, r, to):
        copy = pltpu.make_async_remote_copy(
            src_ref=src, dst_ref=dst, send_sem=s, recv_sem=r, device_id=to, device_id_type=MESH
        )
        copy.start()
        started.append(copy)
        return copy

    from_partner = remote(cc, halo.at[0], halo_s.at[0], halo_r.at[0], partner)
    from_other = remote(cc, halo.at[1], halo_s.at[1], halo_r.at[1], other)
    pass_on(2)

    def spread(src, plane, keep):
        zero_row = jnp.zeros((W, CH), jnp.bfloat16)
        for col in range(3):
            xs[col, plane, 0] = zero_row
            xs[col, plane, H + 1] = zero_row

        @pl.loop(0, 8)
        def _(i):
            v = src[pl.ds(i * 8, 8)].astype(jnp.float32).reshape(8 * W, CH)
            if keep is not None:
                v = jnp.where(keep, v, 0.0)
            w = lax.broadcasted_iota(jnp.int32, (8 * W, CH), 0) % W
            after = jnp.where(w == W - 1, 0.0, pltpu.roll(v, 8 * W - 1, 0))
            before = jnp.where(w == 0, 0.0, pltpu.roll(v, 1, 0))
            for col, moved in ((0, after), (1, v), (2, before)):
                xs[col, plane, pl.ds(1 + i * 8, 8)] = moved.reshape(8, W, CH).astype(jnp.bfloat16)

    def taps(a):
        @pl.loop(0, 3)
        def _(b):
            right = jnp.concatenate(
                [xs[col, 2 - a, pl.ds(2 - b, H)].reshape(POS, CH) for col in range(3)], axis=1
            )
            raw = jnp.dot(act_t[...], right, preferred_element_type=jnp.float32)
            for col in range(3):
                row = pl.multiple_of(((a * 3 + b) * 3 + col) * CH, CH)
                flat[pl.ds(row, CH)] = raw[:, col * CH : (col + 1) * CH]

    loads[2].wait()
    act_t[...] = act[...].reshape(POS, CH).astype(jnp.float32).T.astype(jnp.bfloat16)
    spread(cc, 1, None)
    taps(1)
    pass_on(3)
    from_partner.wait_recv()
    spread(halo.at[0], 2 * (1 - c), None)
    taps(2 * c)
    pass_on(4)
    from_other.wait_recv()
    spread(halo.at[1], 2 * c, jnp.where(c == 0, p > 0, p < n_depth - 1))
    taps(2 - 2 * c)
    pass_on(5)

    core_copies = {}
    for k in (2, 1, 3, 0):
        xx = xk[k]

        @pl.loop(0, NY)
        def _(yy):
            give[xx, yy, 0:ROWS] = flat[pl.ds(((xx * NY + yy) * NC + 1 - c) * ROWS, ROWS)]

        core_copies[k] = remote(give.at[xx], r0.at[xx], r0_s.at[k], r0_r.at[k], partner)

    def both_cores(k):
        xx = xk[k]
        core_copies[k].wait_recv()

        @pl.loop(0, NY)
        def _(yy):
            own = flat[pl.ds(((xx * NY + yy) * NC + c) * ROWS, ROWS)]
            s1[xx, yy, 0:ROWS] = own + r0[xx, yy, 0:ROWS]

    order = (4, 3, 5, 2, 6, 1, 7, 0)
    by_down = {k: i % 2 == 0 for i, k in enumerate(order)}
    yk = [lax.rem(y + k, NY) for k in range(NY)]
    relays, nears, sums = {}, {}, {}
    both_cores(2)
    for k in order:
        to = x_dn if by_down[k] else x_up
        relays[k] = remote(s1.at[xk[2], yk[k]], rel.at[k], rel_s.at[k], rel_r.at[k], to)
    both_cores(1)
    both_cores(3)

    def near(k):
        if by_down[k]:
            nears[k] = remote(s1.at[xk[1], yk[k]], r1.at[0, k], near_s.at[k], near_r.at[k], x_up)
        else:
            nears[k] = remote(s1.at[xk[3], yk[k]], r1.at[1, k], near_s.at[k], near_r.at[k], x_dn)

    near(order[0])
    near(order[1])
    both_cores(0)

    loads[3].wait()

    @pl.loop(0, 4)
    def _(m):
        acc = jnp.zeros((POS // 4, CH), jnp.float32)
        for a in range(3):
            for b in range(3):
                left = jnp.concatenate(
                    [
                        xs[col, 2 - a, pl.ds(2 - b + m * (H // 4), H // 4)].reshape(POS // 4, CH)
                        for col in range(3)
                    ],
                    axis=1,
                )
                right = jnp.concatenate([wts[(a * 3 + b) * 3 + col] for col in range(3)], axis=1)
                acc = acc + lax.dot_general(
                    left, right, (((1,), (1,)), ((), ())), preferred_element_type=jnp.float32
                )
        gi_ref[pl.ds(m * (H // 4), H // 4)] = acc.reshape(H // 4, W, CH).astype(jnp.bfloat16)

    y_copies = {}

    def root(k):
        nears[k].wait_recv()
        sums[k].wait_recv()
        s2[k] = s1[x, yk[k]] + r1[0, k] + r1[1, k]
        if k:
            y_copies[k] = remote(
                s2.at[k], r2.at[k - 1], r2_s.at[k - 1], r2_r.at[k - 1], y_peer[k]
            )

    for i, k in enumerate(order):
        if i + 2 < NY:
            near(order[i + 2])
        relays[k].wait_recv()
        if by_down[k]:
            relayed[k] = s1[xk[3], yk[k]] + rel[k]
            sums[k] = remote(relayed.at[k], r1.at[1, k], sum_s.at[k], sum_r.at[k], x_dn)
        else:
            relayed[k] = s1[xk[1], yk[k]] + rel[k]
            sums[k] = remote(relayed.at[k], r1.at[0, k], sum_s.at[k], sum_r.at[k], x_up)
        if i >= 3:
            root(order[i - 3])
    for k in order[-3:]:
        root(k)

    total = s2[0]
    for k in (7, 1, 6, 2, 5, 3, 4):
        y_copies[k].wait_recv()
        total = total + r2[k - 1]
    s3[...] = total

    for zz in range(NZ):
        win[zz] = s3[first_row(zz) : first_row(zz) + 8]
    far_first = (4, 3, 5, 2, 6, 1, 7)
    z_copies = [
        remote(win.at[lax.rem(z + k, NZ)], r3.at[k - 1], r3_s.at[k - 1], r3_r.at[k - 1], z_peer[k])
        for k in far_first
    ]
    for copy in z_copies:
        copy.wait_recv()
    raw = win[z]
    for k in range(1, NZ):
        raw = raw + r3[k - 1]

    for load in loads[4:]:
        load.wait()
    off = lax.rem(96 * z, 128)
    lane = lax.broadcasted_iota(jnp.int32, (8, CH), 1)
    row = lax.broadcasted_iota(jnp.int32, (8, CH), 0)
    turned = pltpu.roll(raw, lax.rem(128 - off, 128), 1)
    raw = jnp.where(lane < 128 - off, turned, pltpu.roll(turned, 7, 0))
    filter_grad = raw * jnp.float32(1.0 / COUNT**0.5)

    def wide(ref):
        return jnp.concatenate([ref[...], jnp.zeros((8 * CH - SHARE,), jnp.float32)]).reshape(8, CH)

    new_moment = 0.9 * wide(mo) + 0.1 * filter_grad
    new_second = 0.999 * wide(se) + 0.001 * filter_grad * filter_grad
    new_master = wide(ma) - 0.01 * (new_moment / first_fix) / (
        jnp.sqrt(new_second / second_fix) + 1e-08
    )

    turned = pltpu.roll(new_master, off, 1)
    moved = jnp.where(lane >= off, turned, pltpu.roll(turned, 1, 0))
    place = row * CH + lane
    mine = jnp.where((place >= off) & (place < off + SHARE), moved, 0.0)
    out_win[...] = mine
    r4[z] = mine
    share_copies = [
        remote(out_win, r4.at[z], r4_s.at[k - 1], r4_r.at[k - 1], z_peer[k]) for k in far_first
    ]
    fg_ref[...] = filter_grad
    nm_ref[...] = new_moment
    ns_ref[...] = new_second
    nma_ref[...] = new_master
    block[...] = jnp.zeros_like(block)
    for copy in share_copies:
        copy.wait_recv()
    for zz in range(NZ):
        part = pl.ds(first_row(zz), 8)
        block[part] = block[part] + r4[zz]
    full[c, x, y] = block[0:PAD].astype(jnp.bfloat16)

    gather_y = {}
    for k in far_first:
        gather_y[k] = remote(
            full.at[c, x, y], full.at[c, x, y], y_s.at[k - 1], y_r.at[k - 1], y_peer[k]
        )
    near_first = (0, 1, 7, 2, 6, 3, 5, 4)
    up, down, onward, gather_c = {}, {}, {}, {}

    def to_partner(k):
        part = full.at[c, xk[k]]
        gather_c[k] = remote(part, part, c_s.at[k], c_r.at[k], partner)

    src_y = [lax.rem(y + NY - k, NY) for k in range(NY)]
    for k in near_first:
        if k:
            gather_y[k].wait_recv()
        part = full.at[c, x, src_y[k]]
        up[k] = remote(part, part, up_s.at[k], up_r.at[k], x_up)
        down[k] = remote(part, part, dn_s.at[k], dn_r.at[k], x_dn)
        if k in (3, 5, 4):
            onward[k] = remote(part, part, fw_s.at[k], fw_r.at[k], x_far)
    to_partner(0)
    for i, k in enumerate(near_first):
        up[k].wait_recv()
        down[k].wait_recv()
        if k in onward:
            continue
        if i % 2 == 0:
            part = full.at[c, xk[3], src_y[k]]
            onward[k] = remote(part, part, fw_s.at[k], fw_r.at[k], x_up)
        else:
            part = full.at[c, xk[1], src_y[k]]
            onward[k] = remote(part, part, fw_s.at[k], fw_r.at[k], x_dn)
    to_partner(3)
    to_partner(1)

    def lay_out(k):
        xx = xk[k]
        gather_c[k].wait_recv()
        for yy in range(NY):
            for cr in range(NC):
                start = (yy * NC + cr) * ROWS
                nw_ref[xx, start : start + ROWS] = full[cr, xx, yy, 0:ROWS]

    lay_out(0)
    lay_out(3)
    lay_out(1)
    for k in near_first:
        onward[k].wait_recv()
    to_partner(2)
    lay_out(2)

    for copy in started:
        copy.wait_send()


def write_kernel(gi, fg, nm, ns, nma, nw, gi_o, fg_o, nm_o, ns_o, nma_o, nw_o, sem):
    copies = [
        pltpu.make_async_copy(src, dst, sem.at[i])
        for i, (src, dst) in enumerate(
            ((nw, nw_o), (gi, gi_o), (fg, fg_o), (nm, nm_o), (ns, ns_o), (nma, nma_o))
        )
    ]
    for copy in copies:
        copy.start()
    for copy in copies:
        copy.wait()


def step(*operands):
    vmem = pl.BlockSpec(memory_space=pltpu.VMEM)
    hbm = pl.BlockSpec(memory_space=pltpu.HBM)
    f32, bf16 = jnp.float32, jnp.bfloat16
    shape = jax.ShapeDtypeStruct

    def dma(n):
        return pltpu.SemaphoreType.DMA((n,))

    plane = pltpu.VMEM((H, W, CH), bf16)
    return pl.pallas_call(
        kernel,
        out_shape=(
            shape((H, W, CH), bf16),
            shape((8, CH), f32),
            shape((8, CH), f32),
            shape((8, CH), f32),
            shape((8, CH), f32),
            shape((NX, NY * NC * ROWS, CH), bf16),
        ),
        in_specs=[hbm] * 7,
        out_specs=(vmem,) * 6,
        scratch_shapes=[
            plane,
            plane,
            plane,
            pltpu.VMEM((27, CH, CH), bf16),
            pltpu.VMEM((SHARE,), f32),
            pltpu.VMEM((SHARE,), f32),
            pltpu.VMEM((SHARE,), f32),
            dma(7),
            plane,
            pltpu.VMEM((2, H, W, CH), bf16),
            dma(2),
            dma(2),
            pltpu.SemaphoreType.REGULAR((5, 3)),
            pltpu.VMEM((3, 3, H + 2, W, CH), bf16),
            pltpu.VMEM((CH, POS), bf16),
            pltpu.VMEM((NX * NY * NC * ROWS, CH), f32),
            pltpu.VMEM((NX, NY, PAD, CH), f32),
            pltpu.VMEM((NX, NY, PAD, CH), f32),
            dma(NX),
            dma(NX),
            pltpu.VMEM((NX, NY, PAD, CH), f32),
            pltpu.VMEM((NY, PAD, CH), f32),
            dma(NY),
            dma(NY),
            pltpu.VMEM((2, NY, PAD, CH), f32),
            dma(NY),
            dma(NY),
            pltpu.VMEM((NY, PAD, CH), f32),
            dma(NY),
            dma(NY),
            pltpu.VMEM((NY, PAD, CH), f32),
            pltpu.VMEM((NY - 1, PAD, CH), f32),
            dma(NY - 1),
            dma(NY - 1),
            pltpu.VMEM((PAD, CH), f32),
            pltpu.VMEM((NZ, 8, CH), f32),
            pltpu.VMEM((NZ - 1, 8, CH), f32),
            dma(NZ - 1),
            dma(NZ - 1),
            pltpu.VMEM((8, CH), f32),
            pltpu.VMEM((NZ, 8, CH), f32),
            dma(NZ - 1),
            dma(NZ - 1),
            pltpu.VMEM((64, CH), f32),
            pltpu.VMEM((NC, NX, NY, PAD, CH), bf16),
            dma(NY - 1),
            dma(NY - 1),
            dma(NY),
            dma(NY),
            dma(NY),
            dma(NY),
            dma(NY),
            dma(NY),
            dma(NX),
            dma(NX),
        ],
        compiler_params=pltpu.CompilerParams(
            collective_id=0, has_side_effects=True, vmem_limit_bytes=40 * 1024 * 1024
        ),
        name="conv_step",
    )(*[pltpu.with_memory_space_constraint(a, pltpu.HBM) for a in operands])


def write(*results):
    return pl.pallas_call(
        write_kernel,
        out_shape=tuple(jax.ShapeDtypeStruct(a.shape, a.dtype) for a in results),
        in_specs=[pl.BlockSpec(memory_space=pltpu.VMEM)] * 6,
        out_specs=(pl.BlockSpec(memory_space=pltpu.HBM),) * 6,
        scratch_shapes=[pltpu.SemaphoreType.DMA((6,))],
        compiler_params=pltpu.CompilerParams(vmem_limit_bytes=4 * 1024 * 1024),
        name="write_out",
    )(*results)


def local(activations, preact, out_grad, weights, master, moment, second):
    plane = (H, W, CH)
    opt = [master, moment, second]
    gi, fg, nm, ns, nma, nw = write(
        *step(
            activations.reshape(plane),
            preact.reshape(plane),
            out_grad.reshape(plane),
            weights.reshape(27, CH, CH),
            *opt,
        )
    )
    own = [a.reshape(-1)[:SHARE] for a in (fg, nm, ns, nma)]
    return (gi.reshape(activations.shape), *own, nw.reshape(weights.shape))


def solution(mesh):
    volume = P("samp", "depth", None, None, None)
    shares = P(("depth", "samp"))
    return jax.shard_map(
        local,
        mesh=mesh,
        in_specs=(volume, volume, volume, P(), shares, shares, shares),
        out_specs=(volume, shares, shares, shares, shares, P()),
        check_vma=False,
    )
```

```python
import jax
import jax.numpy as jnp
from jax import lax
from jax.experimental import pallas as pl
from jax.experimental.pallas import tpu as pltpu
from jax.sharding import PartitionSpec as P

first_fix = 1.0
second_fix = 0.63230457524

NX, NY, NC, NZ = 4, 8, 2, 8
H, W, CH = 64, 16, 128
POS = H * W
ROWS = 54
PAD = 56
SHARE = 864
COUNT = 8 * 64 * H * W
MESH = pl.DeviceIdType.MESH


def first_row(z):
    return (27 * z) // 4


def kernel(
    act_hbm, pre_hbm, og_hbm, w_hbm, ma_hbm, mo_hbm, se_hbm,
    gi_ref, fg_ref, nm_ref, ns_ref, nma_ref, nw_ref,
    act, pre, og, wts, ma, mo, se, in_sem,
    cc, halo, halo_s, halo_r, known,
    xs, act_t, flat, give,
    r0, r0_s, r0_r,
    s1, r1, x1_s, x1_r,
    s2, r2, r2_s, r2_r,
    s3, win, r3, r3_s, r3_r,
    out_win, r4, r4_s, r4_r, block,
    full, y_s, y_r, up_s, up_r, dn_s, dn_r, fw_s, fw_r, c_s, c_r,
):
    p = lax.axis_index("depth")
    z = lax.axis_index("samp")
    n_depth = NX * NY * NC
    c = lax.rem(p, NC)
    y = lax.rem(p // NC, NY)
    x = p // (NC * NY)

    def dev(xx, yy, ccore, zz):
        return {"depth": (xx * NY + yy) * NC + ccore, "samp": zz}

    partner = dev(x, y, 1 - c, z)
    other = {"depth": lax.rem(p + n_depth + 2 * c - 1, n_depth), "samp": z}
    xk = [lax.rem(x + k, NX) for k in range(NX)]
    x_up = dev(xk[1], y, c, z)
    x_far = dev(xk[2], y, c, z)
    x_dn = dev(xk[3], y, c, z)
    y_peer = [dev(x, lax.rem(y + k, NY), c, z) for k in range(NY)]
    z_peer = [dev(x, y, c, lax.rem(z + k, NZ)) for k in range(NZ)]

    loads = [
        pltpu.make_async_copy(src, dst, in_sem.at[i])
        for i, (src, dst) in enumerate(
            (
                (pre_hbm, pre),
                (og_hbm, og),
                (act_hbm, act),
                (w_hbm, wts),
                (ma_hbm, ma),
                (mo_hbm, mo),
                (se_hbm, se),
            )
        )
    ]
    for load in loads:
        load.start()

    barrier = pltpu.get_barrier_semaphore()
    peers = [partner, other, x_up, x_dn, y_peer[1], y_peer[7], z_peer[1], z_peer[7]]
    for peer in peers:
        pl.semaphore_signal(barrier, inc=1, device_id=peer, device_id_type=MESH)

    loads[0].wait()
    loads[1].wait()

    @pl.loop(0, 8)
    def _(i):
        part = pl.ds(i * 8, 8)
        slope = jnp.where(pre[part].astype(jnp.float32) > 0, jnp.float32(1.0), jnp.float32(0.01))
        cc[part] = (og[part].astype(jnp.float32) * slope).astype(jnp.bfloat16)

    pl.semaphore_wait(barrier, len(peers))

    flows = ((y_peer[1], 3), (y_peer[7], 4), (z_peer[1], 3), (z_peer[7], 4), (x_up, 2))

    def pass_on(hops):
        for i, (_, last) in enumerate(flows):
            if 2 < hops <= last + 1:
                pl.semaphore_wait(known.at[i, hops - 3], 1)
        for i, (to, last) in enumerate(flows):
            if hops <= last:
                pl.semaphore_signal(
                    known.at[i, hops - 2], inc=1, device_id=to, device_id_type=MESH
                )

    started = []

    def remote(src, dst, s, r, to):
        copy = pltpu.make_async_remote_copy(
            src_ref=src, dst_ref=dst, send_sem=s, recv_sem=r, device_id=to, device_id_type=MESH
        )
        copy.start()
        started.append(copy)
        return copy

    from_partner = remote(cc, halo.at[0], halo_s.at[0], halo_r.at[0], partner)
    from_other = remote(cc, halo.at[1], halo_s.at[1], halo_r.at[1], other)
    pass_on(2)

    def spread(src, plane, keep):
        zero_row = jnp.zeros((W, CH), jnp.bfloat16)
        for col in range(3):
            xs[col, plane, 0] = zero_row
            xs[col, plane, H + 1] = zero_row

        @pl.loop(0, 8)
        def _(i):
            v = src[pl.ds(i * 8, 8)].astype(jnp.float32).reshape(8 * W, CH)
            if keep is not None:
                v = jnp.where(keep, v, 0.0)
            w = lax.broadcasted_iota(jnp.int32, (8 * W, CH), 0) % W
            after = jnp.where(w == W - 1, 0.0, pltpu.roll(v, 8 * W - 1, 0))
            before = jnp.where(w == 0, 0.0, pltpu.roll(v, 1, 0))
            for col, moved in ((0, after), (1, v), (2, before)):
                xs[col, plane, pl.ds(1 + i * 8, 8)] = moved.reshape(8, W, CH).astype(jnp.bfloat16)

    def taps(a):
        @pl.loop(0, 3)
        def _(b):
            right = jnp.concatenate(
                [xs[col, 2 - a, pl.ds(2 - b, H)].reshape(POS, CH) for col in range(3)], axis=1
            )
            raw = jnp.dot(act_t[...], right, preferred_element_type=jnp.float32)
            for col in range(3):
                row = pl.multiple_of(((a * 3 + b) * 3 + col) * CH, CH)
                flat[pl.ds(row, CH)] = raw[:, col * CH : (col + 1) * CH]

    def exchange(group, first, count):
        @pl.loop(0, count)
        def _(j):
            q = first + j
            give[q, 0:ROWS] = flat[pl.ds((q * NC + 1 - c) * ROWS, ROWS)]

        part = pl.ds(first, count)
        return remote(give.at[part], r0.at[part], r0_s.at[group], r0_r.at[group], partner)

    def both_cores(first, count):
        @pl.loop(0, count)
        def _(j):
            q = first + j
            own = flat[pl.ds((q * NC + c) * ROWS, ROWS)]
            s1[q, 0:ROWS] = own + r0[q, 0:ROWS]

    loads[2].wait()
    act_t[...] = act[...].reshape(POS, CH).astype(jnp.float32).T.astype(jnp.bfloat16)
    spread(cc, 1, None)
    taps(1)
    middle = exchange(0, 11, 10)
    pass_on(3)
    from_partner.wait_recv()
    spread(halo.at[0], 2 * (1 - c), None)
    taps(2 * c)
    early = exchange(1, 21 * c, 11)
    middle.wait_recv()
    both_cores(11, 10)
    pass_on(4)
    from_other.wait_recv()
    spread(halo.at[1], 2 * c, jnp.where(c == 0, p > 0, p < n_depth - 1))
    taps(2 - 2 * c)
    late = exchange(2, 21 * (1 - c), 11)
    early.wait_recv()
    both_cores(21 * (1 - c), 11)
    pass_on(5)
    late.wait_recv()
    both_cores(21 * c, 11)

    order = (4, 3, 5, 2, 6, 1, 7, 0)
    yk = [lax.rem(y + k, NY) for k in range(NY)]
    x_copies = {}
    for k in order:
        x_copies[k] = [
            remote(
                s1.at[xk[j] * NY + yk[k]],
                r1.at[j - 1, k],
                x1_s.at[j - 1, k],
                x1_r.at[j - 1, k],
                to,
            )
            for j, to in ((2, x_far), (1, x_up), (3, x_dn))
        ]

    loads[3].wait()

    @pl.loop(0, 4)
    def _(m):
        acc = jnp.zeros((POS // 4, CH), jnp.float32)
        for a in range(3):
            for b in range(3):
                left = jnp.concatenate(
                    [
                        xs[col, 2 - a, pl.ds(2 - b + m * (H // 4), H // 4)].reshape(POS // 4, CH)
                        for col in range(3)
                    ],
                    axis=1,
                )
                right = jnp.concatenate([wts[(a * 3 + b) * 3 + col] for col in range(3)], axis=1)
                acc = acc + lax.dot_general(
                    left, right, (((1,), (1,)), ((), ())), preferred_element_type=jnp.float32
                )
        gi_ref[pl.ds(m * (H // 4), H // 4)] = acc.reshape(H // 4, W, CH).astype(jnp.bfloat16)

    y_copies = {}

    for k in order:
        for copy in x_copies[k]:
            copy.wait_recv()
        s2[k] = s1[x * NY + yk[k]] + r1[0, k] + r1[1, k] + r1[2, k]
        if k:
            y_copies[k] = remote(
                s2.at[k], r2.at[k - 1], r2_s.at[k - 1], r2_r.at[k - 1], y_peer[k]
            )

    total = s2[0]
    for k in (7, 1, 6, 2, 5, 3, 4):
        y_copies[k].wait_recv()
        total = total + r2[k - 1]
    s3[...] = total

    for zz in range(NZ):
        win[zz] = s3[first_row(zz) : first_row(zz) + 8]
    far_first = (4, 3, 5, 2, 6, 1, 7)
    z_copies = [
        remote(win.at[lax.rem(z + k, NZ)], r3.at[k - 1], r3_s.at[k - 1], r3_r.at[k - 1], z_peer[k])
        for k in far_first
    ]
    for copy in z_copies:
        copy.wait_recv()
    raw = win[z]
    for k in range(1, NZ):
        raw = raw + r3[k - 1]

    for load in loads[4:]:
        load.wait()
    off = lax.rem(96 * z, 128)
    lane = lax.broadcasted_iota(jnp.int32, (8, CH), 1)
    row = lax.broadcasted_iota(jnp.int32, (8, CH), 0)
    turned = pltpu.roll(raw, lax.rem(128 - off, 128), 1)
    raw = jnp.where(lane < 128 - off, turned, pltpu.roll(turned, 7, 0))
    filter_grad = raw * jnp.float32(1.0 / COUNT**0.5)

    def wide(ref):
        return jnp.concatenate([ref[...], jnp.zeros((8 * CH - SHARE,), jnp.float32)]).reshape(8, CH)

    new_moment = 0.9 * wide(mo) + 0.1 * filter_grad
    new_second = 0.999 * wide(se) + 0.001 * filter_grad * filter_grad
    new_master = wide(ma) - 0.01 * (new_moment / first_fix) / (
        jnp.sqrt(new_second / second_fix) + 1e-08
    )

    turned = pltpu.roll(new_master, off, 1)
    moved = jnp.where(lane >= off, turned, pltpu.roll(turned, 1, 0))
    place = row * CH + lane
    mine = jnp.where((place >= off) & (place < off + SHARE), moved, 0.0)
    mine = mine.astype(jnp.bfloat16)
    out_win[...] = mine
    r4[z] = mine
    share_copies = [
        remote(out_win, r4.at[z], r4_s.at[k - 1], r4_r.at[k - 1], z_peer[k]) for k in far_first
    ]
    fg_ref[...] = filter_grad
    nm_ref[...] = new_moment
    ns_ref[...] = new_second
    nma_ref[...] = new_master
    block[...] = jnp.zeros_like(block)
    for copy in share_copies:
        copy.wait_recv()
    for zz in range(NZ):
        part = pl.ds(first_row(zz), 8)
        block[part] = block[part] + r4[zz].astype(jnp.float32)
    full[c, x, y] = block[0:PAD].astype(jnp.bfloat16)

    gather_y = {}
    for k in far_first:
        gather_y[k] = remote(
            full.at[c, x, y], full.at[c, x, y], y_s.at[k - 1], y_r.at[k - 1], y_peer[k]
        )
    near_first = (0, 1, 7, 2, 6, 3, 5, 4)
    up, down, onward, gather_c = {}, {}, {}, {}

    def to_partner(k):
        part = full.at[c, xk[k]]
        gather_c[k] = remote(part, part, c_s.at[k], c_r.at[k], partner)

    src_y = [lax.rem(y + NY - k, NY) for k in range(NY)]
    for k in near_first:
        if k:
            gather_y[k].wait_recv()
        part = full.at[c, x, src_y[k]]
        up[k] = remote(part, part, up_s.at[k], up_r.at[k], x_up)
        down[k] = remote(part, part, dn_s.at[k], dn_r.at[k], x_dn)
        onward[k] = remote(part, part, fw_s.at[k], fw_r.at[k], x_far)
    to_partner(0)
    for k in near_first:
        up[k].wait_recv()
        down[k].wait_recv()
    to_partner(3)
    to_partner(1)

    def lay_out(k):
        xx = xk[k]
        gather_c[k].wait_recv()
        for yy in range(NY):
            for cr in range(NC):
                start = (yy * NC + cr) * ROWS
                nw_ref[xx, start : start + ROWS] = full[cr, xx, yy, 0:ROWS]

    lay_out(0)
    lay_out(3)
    lay_out(1)
    for k in near_first:
        onward[k].wait_recv()
    to_partner(2)
    lay_out(2)

    for copy in started:
        copy.wait_send()


def write_kernel(gi, fg, nm, ns, nma, nw, gi_o, fg_o, nm_o, ns_o, nma_o, nw_o, sem):
    copies = [
        pltpu.make_async_copy(src, dst, sem.at[i])
        for i, (src, dst) in enumerate(
            ((nw, nw_o), (gi, gi_o), (fg, fg_o), (nm, nm_o), (ns, ns_o), (nma, nma_o))
        )
    ]
    for copy in copies:
        copy.start()
    for copy in copies:
        copy.wait()


def step(*operands):
    vmem = pl.BlockSpec(memory_space=pltpu.VMEM)
    hbm = pl.BlockSpec(memory_space=pltpu.HBM)
    f32, bf16 = jnp.float32, jnp.bfloat16
    shape = jax.ShapeDtypeStruct

    def dma(n):
        return pltpu.SemaphoreType.DMA((n,))

    plane = pltpu.VMEM((H, W, CH), bf16)
    return pl.pallas_call(
        kernel,
        out_shape=(
            shape((H, W, CH), bf16),
            shape((8, CH), f32),
            shape((8, CH), f32),
            shape((8, CH), f32),
            shape((8, CH), f32),
            shape((NX, NY * NC * ROWS, CH), bf16),
        ),
        in_specs=[hbm] * 7,
        out_specs=(vmem,) * 6,
        scratch_shapes=[
            plane,
            plane,
            plane,
            pltpu.VMEM((27, CH, CH), bf16),
            pltpu.VMEM((SHARE,), f32),
            pltpu.VMEM((SHARE,), f32),
            pltpu.VMEM((SHARE,), f32),
            dma(7),
            plane,
            pltpu.VMEM((2, H, W, CH), bf16),
            dma(2),
            dma(2),
            pltpu.SemaphoreType.REGULAR((5, 3)),
            pltpu.VMEM((3, 3, H + 2, W, CH), bf16),
            pltpu.VMEM((CH, POS), bf16),
            pltpu.VMEM((NX * NY * NC * ROWS, CH), f32),
            pltpu.VMEM((NX * NY, PAD, CH), f32),
            pltpu.VMEM((NX * NY, PAD, CH), f32),
            dma(3),
            dma(3),
            pltpu.VMEM((NX * NY, PAD, CH), f32),
            pltpu.VMEM((NX - 1, NY, PAD, CH), f32),
            pltpu.SemaphoreType.DMA((NX - 1, NY)),
            pltpu.SemaphoreType.DMA((NX - 1, NY)),
            pltpu.VMEM((NY, PAD, CH), f32),
            pltpu.VMEM((NY - 1, PAD, CH), f32),
            dma(NY - 1),
            dma(NY - 1),
            pltpu.VMEM((PAD, CH), f32),
            pltpu.VMEM((NZ, 8, CH), f32),
            pltpu.VMEM((NZ - 1, 8, CH), f32),
            dma(NZ - 1),
            dma(NZ - 1),
            pltpu.VMEM((8, CH), bf16),
            pltpu.VMEM((NZ, 8, CH), bf16),
            dma(NZ - 1),
            dma(NZ - 1),
            pltpu.VMEM((64, CH), f32),
            pltpu.VMEM((NC, NX, NY, PAD, CH), bf16),
            dma(NY - 1),
            dma(NY - 1),
            dma(NY),
            dma(NY),
            dma(NY),
            dma(NY),
            dma(NY),
            dma(NY),
            dma(NX),
            dma(NX),
        ],
        compiler_params=pltpu.CompilerParams(
            collective_id=0, has_side_effects=True, vmem_limit_bytes=40 * 1024 * 1024
        ),
        name="conv_step",
    )(*[pltpu.with_memory_space_constraint(a, pltpu.HBM) for a in operands])


def write(*results):
    return pl.pallas_call(
        write_kernel,
        out_shape=tuple(jax.ShapeDtypeStruct(a.shape, a.dtype) for a in results),
        in_specs=[pl.BlockSpec(memory_space=pltpu.VMEM)] * 6,
        out_specs=(pl.BlockSpec(memory_space=pltpu.HBM),) * 6,
        scratch_shapes=[pltpu.SemaphoreType.DMA((6,))],
        compiler_params=pltpu.CompilerParams(vmem_limit_bytes=4 * 1024 * 1024),
        name="write_out",
    )(*results)


def local(activations, preact, out_grad, weights, master, moment, second):
    plane = (H, W, CH)
    opt = [master, moment, second]
    gi, fg, nm, ns, nma, nw = write(
        *step(
            activations.reshape(plane),
            preact.reshape(plane),
            out_grad.reshape(plane),
            weights.reshape(27, CH, CH),
            *opt,
        )
    )
    own = [a.reshape(-1)[:SHARE] for a in (fg, nm, ns, nma)]
    return (gi.reshape(activations.shape), *own, nw.reshape(weights.shape))


def solution(mesh):
    volume = P("samp", "depth", None, None, None)
    shares = P(("depth", "samp"))
    return jax.shard_map(
        local,
        mesh=mesh,
        in_specs=(volume, volume, volume, P(), shares, shares, shares),
        out_specs=(volume, shares, shares, shares, shares, P()),
        check_vma=False,
    )
```

```python
import jax
import jax.numpy as jnp
from jax import lax
from jax.experimental import pallas as pl
from jax.experimental.pallas import tpu as pltpu
from jax.sharding import PartitionSpec as P

first_fix = 1.0
second_fix = 0.63230457524

NX, NY, NC, NZ = 4, 8, 2, 8
H, W, CH = 64, 16, 128
POS = H * W
ROWS = 54
PAD = 56
SHARE = 864
COUNT = 8 * 64 * H * W
MESH = pl.DeviceIdType.MESH


def first_row(z):
    return (27 * z) // 4


def kernel(
    act_hbm, pre_hbm, og_hbm, w_hbm, ma_hbm, mo_hbm, se_hbm,
    gi_ref, fg_ref, nm_ref, ns_ref, nma_ref, nw_ref,
    act, pre, og, wts, ma, mo, se, in_sem,
    cc, halo, halo_s, halo_r, known,
    xs, act_t, flat, give,
    r0, r0_s, r0_r,
    s1, r1, x1_s, x1_r,
    s2, r2, r2_s, r2_r,
    s3, win, r3, r3_s, r3_r,
    out_win, r4, r4_s, r4_r, block,
    full, y_s, y_r, up_s, up_r, dn_s, dn_r, fw_s, fw_r, c_s, c_r,
):
    p = lax.axis_index("depth")
    z = lax.axis_index("samp")
    n_depth = NX * NY * NC
    c = lax.rem(p, NC)
    y = lax.rem(p // NC, NY)
    x = p // (NC * NY)

    def dev(xx, yy, ccore, zz):
        return {"depth": (xx * NY + yy) * NC + ccore, "samp": zz}

    partner = dev(x, y, 1 - c, z)
    other = {"depth": lax.rem(p + n_depth + 2 * c - 1, n_depth), "samp": z}
    xk = [lax.rem(x + k, NX) for k in range(NX)]
    x_up = dev(xk[1], y, c, z)
    x_far = dev(xk[2], y, c, z)
    x_dn = dev(xk[3], y, c, z)
    y_peer = [dev(x, lax.rem(y + k, NY), c, z) for k in range(NY)]
    z_peer = [dev(x, y, c, lax.rem(z + k, NZ)) for k in range(NZ)]

    loads = [
        pltpu.make_async_copy(src, dst, in_sem.at[i])
        for i, (src, dst) in enumerate(
            (
                (pre_hbm, pre),
                (og_hbm, og),
                (act_hbm, act),
                (w_hbm, wts),
                (ma_hbm, ma),
                (mo_hbm, mo),
                (se_hbm, se),
            )
        )
    ]
    for load in loads:
        load.start()

    barrier = pltpu.get_barrier_semaphore()
    peers = [partner, other, x_up, x_dn, y_peer[1], y_peer[7], z_peer[1], z_peer[7]]
    for peer in peers:
        pl.semaphore_signal(barrier, inc=1, device_id=peer, device_id_type=MESH)

    loads[0].wait()
    loads[1].wait()

    @pl.loop(0, 8)
    def _(i):
        part = pl.ds(i * 8, 8)
        slope = jnp.where(pre[part].astype(jnp.float32) > 0, jnp.float32(1.0), jnp.float32(0.01))
        cc[part] = (og[part].astype(jnp.float32) * slope).astype(jnp.bfloat16)

    pl.semaphore_wait(barrier, len(peers))

    flows = ((y_peer[1], 3), (y_peer[7], 4), (z_peer[1], 3), (z_peer[7], 4), (x_up, 2))

    def pass_on(hops):
        for i, (_, last) in enumerate(flows):
            if 2 < hops <= last + 1:
                pl.semaphore_wait(known.at[i, hops - 3], 1)
        for i, (to, last) in enumerate(flows):
            if hops <= last:
                pl.semaphore_signal(
                    known.at[i, hops - 2], inc=1, device_id=to, device_id_type=MESH
                )

    started = []

    def remote(src, dst, s, r, to):
        copy = pltpu.make_async_remote_copy(
            src_ref=src, dst_ref=dst, send_sem=s, recv_sem=r, device_id=to, device_id_type=MESH
        )
        copy.start()
        started.append(copy)
        return copy

    from_partner = remote(cc, halo.at[0], halo_s.at[0], halo_r.at[0], partner)
    from_other = remote(cc, halo.at[1], halo_s.at[1], halo_r.at[1], other)
    pass_on(2)

    def spread(src, plane, keep):
        zero_row = jnp.zeros((W, CH), jnp.bfloat16)
        for col in range(3):
            xs[col, plane, 0] = zero_row
            xs[col, plane, H + 1] = zero_row

        @pl.loop(0, 8)
        def _(i):
            v = src[pl.ds(i * 8, 8)].astype(jnp.float32).reshape(8 * W, CH)
            if keep is not None:
                v = jnp.where(keep, v, 0.0)
            w = lax.broadcasted_iota(jnp.int32, (8 * W, CH), 0) % W
            after = jnp.where(w == W - 1, 0.0, pltpu.roll(v, 8 * W - 1, 0))
            before = jnp.where(w == 0, 0.0, pltpu.roll(v, 1, 0))
            for col, moved in ((0, after), (1, v), (2, before)):
                xs[col, plane, pl.ds(1 + i * 8, 8)] = moved.reshape(8, W, CH).astype(jnp.bfloat16)

    def taps(a):
        @pl.loop(0, 3)
        def _(b):
            right = jnp.concatenate(
                [xs[col, 2 - a, pl.ds(2 - b, H)].reshape(POS, CH) for col in range(3)], axis=1
            )
            raw = jnp.dot(act_t[...], right, preferred_element_type=jnp.float32)
            for col in range(3):
                row = pl.multiple_of(((a * 3 + b) * 3 + col) * CH, CH)
                flat[pl.ds(row, CH)] = raw[:, col * CH : (col + 1) * CH]

    def exchange(group, first, count):
        @pl.loop(0, count)
        def _(j):
            q = first + j
            give[q, 0:ROWS] = flat[pl.ds((q * NC + 1 - c) * ROWS, ROWS)]

        part = pl.ds(first, count)
        return remote(give.at[part], r0.at[part], r0_s.at[group], r0_r.at[group], partner)

    def both_cores(first, count):
        @pl.loop(0, count)
        def _(j):
            q = first + j
            own = flat[pl.ds((q * NC + c) * ROWS, ROWS)]
            s1[q, 0:ROWS] = own + r0[q, 0:ROWS]

    loads[2].wait()
    act_t[...] = act[...].reshape(POS, CH).astype(jnp.float32).T.astype(jnp.bfloat16)
    spread(cc, 1, None)
    taps(1)
    middle = exchange(0, 11, 10)
    pass_on(3)
    from_partner.wait_recv()
    spread(halo.at[0], 2 * (1 - c), None)
    taps(2 * c)
    early = exchange(1, 21 * c, 11)
    middle.wait_recv()
    both_cores(11, 10)
    pass_on(4)
    from_other.wait_recv()
    spread(halo.at[1], 2 * c, jnp.where(c == 0, p > 0, p < n_depth - 1))
    taps(2 - 2 * c)
    late = exchange(2, 21 * (1 - c), 11)
    early.wait_recv()
    both_cores(21 * (1 - c), 11)
    pass_on(5)
    late.wait_recv()
    both_cores(21 * c, 11)

    order = (4, 3, 5, 2, 6, 1, 7, 0)
    yk = [lax.rem(y + k, NY) for k in range(NY)]
    x_copies = {}
    for k in order:
        x_copies[k] = [
            remote(
                s1.at[xk[j] * NY + yk[k]],
                r1.at[j - 1, k],
                x1_s.at[j - 1, k],
                x1_r.at[j - 1, k],
                to,
            )
            for j, to in ((2, x_far), (1, x_up), (3, x_dn))
        ]

    loads[3].wait()

    @pl.loop(0, 4)
    def _(m):
        acc = jnp.zeros((POS // 4, CH), jnp.float32)
        for a in range(3):
            for b in range(3):
                left = jnp.concatenate(
                    [
                        xs[col, 2 - a, pl.ds(2 - b + m * (H // 4), H // 4)].reshape(POS // 4, CH)
                        for col in range(3)
                    ],
                    axis=1,
                )
                right = jnp.concatenate([wts[(a * 3 + b) * 3 + col] for col in range(3)], axis=1)
                acc = acc + lax.dot_general(
                    left, right, (((1,), (1,)), ((), ())), preferred_element_type=jnp.float32
                )
        gi_ref[pl.ds(m * (H // 4), H // 4)] = acc.reshape(H // 4, W, CH).astype(jnp.bfloat16)

    y_copies = {}

    for k in order:
        for copy in x_copies[k]:
            copy.wait_recv()
        s2[k] = s1[x * NY + yk[k]] + r1[0, k] + r1[1, k] + r1[2, k]
        if k:
            y_copies[k] = remote(
                s2.at[k], r2.at[k - 1], r2_s.at[k - 1], r2_r.at[k - 1], y_peer[k]
            )

    total = s2[0]
    for k in (7, 1, 6, 2, 5, 3, 4):
        y_copies[k].wait_recv()
        total = total + r2[k - 1]
    s3[...] = total

    for zz in range(NZ):
        win[zz] = s3[first_row(zz) : first_row(zz) + 8]
    far_first = (4, 3, 5, 2, 6, 1, 7)
    z_copies = [
        remote(win.at[lax.rem(z + k, NZ)], r3.at[k - 1], r3_s.at[k - 1], r3_r.at[k - 1], z_peer[k])
        for k in far_first
    ]
    for copy in z_copies:
        copy.wait_recv()
    raw = win[z]
    for k in range(1, NZ):
        raw = raw + r3[k - 1]

    for load in loads[4:]:
        load.wait()
    off = lax.rem(96 * z, 128)
    lane = lax.broadcasted_iota(jnp.int32, (8, CH), 1)
    row = lax.broadcasted_iota(jnp.int32, (8, CH), 0)
    turned = pltpu.roll(raw, lax.rem(128 - off, 128), 1)
    raw = jnp.where(lane < 128 - off, turned, pltpu.roll(turned, 7, 0))
    filter_grad = raw * jnp.float32(1.0 / COUNT**0.5)

    def wide(ref):
        return jnp.concatenate([ref[...], jnp.zeros((8 * CH - SHARE,), jnp.float32)]).reshape(8, CH)

    new_moment = 0.9 * wide(mo) + 0.1 * filter_grad
    new_second = 0.999 * wide(se) + 0.001 * filter_grad * filter_grad
    new_master = wide(ma) - 0.01 * (new_moment / first_fix) / (
        jnp.sqrt(new_second / second_fix) + 1e-08
    )

    turned = pltpu.roll(new_master, off, 1)
    moved = jnp.where(lane >= off, turned, pltpu.roll(turned, 1, 0))
    place = row * CH + lane
    mine = jnp.where((place >= off) & (place < off + SHARE), moved, 0.0)
    mine = mine.astype(jnp.bfloat16)
    out_win[...] = mine
    r4[z] = mine
    share_copies = [
        remote(out_win, r4.at[z], r4_s.at[k - 1], r4_r.at[k - 1], z_peer[k]) for k in far_first
    ]
    fg_ref[...] = filter_grad
    nm_ref[...] = new_moment
    ns_ref[...] = new_second
    nma_ref[...] = new_master
    block[...] = jnp.zeros_like(block)
    for copy in share_copies:
        copy.wait_recv()
    for zz in range(NZ):
        part = pl.ds(first_row(zz), 8)
        block[part] = block[part] + r4[zz].astype(jnp.float32)
    full[c, x, y] = block[0:PAD].astype(jnp.bfloat16)

    gather_y = {}
    for k in far_first:
        gather_y[k] = remote(
            full.at[c, x, y], full.at[c, x, y], y_s.at[k - 1], y_r.at[k - 1], y_peer[k]
        )
    near_first = (0, 1, 7, 2, 6, 3, 5, 4)
    up, down, onward, gather_c = {}, {}, {}, {}

    def to_partner(k):
        part = full.at[c, xk[k]]
        gather_c[k] = remote(part, part, c_s.at[k], c_r.at[k], partner)

    src_y = [lax.rem(y + NY - k, NY) for k in range(NY)]
    for k in near_first:
        if k:
            gather_y[k].wait_recv()
        part = full.at[c, x, src_y[k]]
        onward[k] = remote(part, part, fw_s.at[k], fw_r.at[k], x_far)
        up[k] = remote(part, part, up_s.at[k], up_r.at[k], x_up)
        down[k] = remote(part, part, dn_s.at[k], dn_r.at[k], x_dn)
    to_partner(0)
    for k in near_first:
        up[k].wait_recv()
    to_partner(3)
    for k in near_first:
        down[k].wait_recv()
    to_partner(1)
    for k in near_first:
        onward[k].wait_recv()
    to_partner(2)

    def lay_out(k):
        xx = xk[k]
        gather_c[k].wait_recv()
        for yy in range(NY):
            for cr in range(NC):
                start = (yy * NC + cr) * ROWS
                nw_ref[xx, start : start + ROWS] = full[cr, xx, yy, 0:ROWS]

    lay_out(0)
    lay_out(3)
    lay_out(1)
    lay_out(2)

    for copy in started:
        copy.wait_send()


def write_kernel(gi, fg, nm, ns, nma, nw, gi_o, fg_o, nm_o, ns_o, nma_o, nw_o, sem):
    copies = [
        pltpu.make_async_copy(src, dst, sem.at[i])
        for i, (src, dst) in enumerate(
            ((nw, nw_o), (gi, gi_o), (fg, fg_o), (nm, nm_o), (ns, ns_o), (nma, nma_o))
        )
    ]
    for copy in copies:
        copy.start()
    for copy in copies:
        copy.wait()


def step(*operands):
    vmem = pl.BlockSpec(memory_space=pltpu.VMEM)
    hbm = pl.BlockSpec(memory_space=pltpu.HBM)
    f32, bf16 = jnp.float32, jnp.bfloat16
    shape = jax.ShapeDtypeStruct

    def dma(n):
        return pltpu.SemaphoreType.DMA((n,))

    plane = pltpu.VMEM((H, W, CH), bf16)
    return pl.pallas_call(
        kernel,
        out_shape=(
            shape((H, W, CH), bf16),
            shape((8, CH), f32),
            shape((8, CH), f32),
            shape((8, CH), f32),
            shape((8, CH), f32),
            shape((NX, NY * NC * ROWS, CH), bf16),
        ),
        in_specs=[hbm] * 7,
        out_specs=(vmem,) * 6,
        scratch_shapes=[
            plane,
            plane,
            plane,
            pltpu.VMEM((27, CH, CH), bf16),
            pltpu.VMEM((SHARE,), f32),
            pltpu.VMEM((SHARE,), f32),
            pltpu.VMEM((SHARE,), f32),
            dma(7),
            plane,
            pltpu.VMEM((2, H, W, CH), bf16),
            dma(2),
            dma(2),
            pltpu.SemaphoreType.REGULAR((5, 3)),
            pltpu.VMEM((3, 3, H + 2, W, CH), bf16),
            pltpu.VMEM((CH, POS), bf16),
            pltpu.VMEM((NX * NY * NC * ROWS, CH), f32),
            pltpu.VMEM((NX * NY, PAD, CH), f32),
            pltpu.VMEM((NX * NY, PAD, CH), f32),
            dma(3),
            dma(3),
            pltpu.VMEM((NX * NY, PAD, CH), f32),
            pltpu.VMEM((NX - 1, NY, PAD, CH), f32),
            pltpu.SemaphoreType.DMA((NX - 1, NY)),
            pltpu.SemaphoreType.DMA((NX - 1, NY)),
            pltpu.VMEM((NY, PAD, CH), f32),
            pltpu.VMEM((NY - 1, PAD, CH), f32),
            dma(NY - 1),
            dma(NY - 1),
            pltpu.VMEM((PAD, CH), f32),
            pltpu.VMEM((NZ, 8, CH), f32),
            pltpu.VMEM((NZ - 1, 8, CH), f32),
            dma(NZ - 1),
            dma(NZ - 1),
            pltpu.VMEM((8, CH), bf16),
            pltpu.VMEM((NZ, 8, CH), bf16),
            dma(NZ - 1),
            dma(NZ - 1),
            pltpu.VMEM((64, CH), f32),
            pltpu.VMEM((NC, NX, NY, PAD, CH), bf16),
            dma(NY - 1),
            dma(NY - 1),
            dma(NY),
            dma(NY),
            dma(NY),
            dma(NY),
            dma(NY),
            dma(NY),
            dma(NX),
            dma(NX),
        ],
        compiler_params=pltpu.CompilerParams(
            collective_id=0, has_side_effects=True, vmem_limit_bytes=40 * 1024 * 1024
        ),
        name="conv_step",
    )(*[pltpu.with_memory_space_constraint(a, pltpu.HBM) for a in operands])


def write(*results):
    return pl.pallas_call(
        write_kernel,
        out_shape=tuple(jax.ShapeDtypeStruct(a.shape, a.dtype) for a in results),
        in_specs=[pl.BlockSpec(memory_space=pltpu.VMEM)] * 6,
        out_specs=(pl.BlockSpec(memory_space=pltpu.HBM),) * 6,
        scratch_shapes=[pltpu.SemaphoreType.DMA((6,))],
        compiler_params=pltpu.CompilerParams(vmem_limit_bytes=4 * 1024 * 1024),
        name="write_out",
    )(*results)


def local(activations, preact, out_grad, weights, master, moment, second):
    plane = (H, W, CH)
    opt = [master, moment, second]
    gi, fg, nm, ns, nma, nw = write(
        *step(
            activations.reshape(plane),
            preact.reshape(plane),
            out_grad.reshape(plane),
            weights.reshape(27, CH, CH),
            *opt,
        )
    )
    own = [a.reshape(-1)[:SHARE] for a in (fg, nm, ns, nma)]
    return (gi.reshape(activations.shape), *own, nw.reshape(weights.shape))


def solution(mesh):
    volume = P("samp", "depth", None, None, None)
    shares = P(("depth", "samp"))
    return jax.shard_map(
        local,
        mesh=mesh,
        in_specs=(volume, volume, volume, P(), shares, shares, shares),
        out_specs=(volume, shares, shares, shares, shares, P()),
        check_vma=False,
    )
```
